32 devices in a mesh: side: 8 (over y, x, core), lane: 4 (over z).
Axes of the slice: x: 2, y: 2, z: 4, core: 2. Of those that a mesh axis runs over, the one named last changes fastest.
Arguments:
- tokens: bfloat16 [4096, 2048], P(('side', 'lane')), may hold values from -6 to 6
- expert_ids: int32 [4096, 8], P(('side', 'lane')), may hold values from 0 to 31, all different within a row; in each aligned block of 128 rows (0 to 127, 128 to 255, ...) at most 64 rows name the same one
- route_weights: float32 [4096, 8], P(('side', 'lane')), may hold values from 0.03 to 0.4
- w_gate: bfloat16 [32, 2048, 768], P(('side', 'lane')), may hold values from -0.125 to 0.125
- w_up: bfloat16 [32, 2048, 768], P(('side', 'lane')), may hold values from -0.125 to 0.125
- w_down: bfloat16 [32, 768, 2048], P(('side', 'lane')), may hold values from -0.21875 to 0.21875
Outputs:
- mixed: bfloat16 [4096, 2048], P(('side', 'lane'))
The draws below stay inside these ranges and needn't reach their ends.
Inputs may be any that keep to these rules, and one draw needn't show every extreme that they name: `expert_ids`: each row names 8 different experts. Within each aligned block of 128 rows (the rows of one device) no expert is named by more than 64 rows, and in every draw some expert is named by exactly 64 rows of some block.
All inputs are finite; a program needn't handle non-finite values.
Results may differ from the reference program's by a relative error of at most 0.0085.
Values may be sent and summed in bfloat16 or wider, within the bound.
A program may use at most 128 MiB of HBM per device.

```python
import math
import jax
import jax.numpy as jnp
import numpy as np
from jax import lax

D = 2048
FFE = 768
TOP = 8
TOK_DEV = 128
EXPERTS = 32
TOKENS = 4096
CAP = 64


def steps_of(rng, dims, cuts, smallest, top_value):
    def one(position, shards_of):
        heights = jax.random.uniform(jax.random.fold_in(jax.random.fold_in(rng, 6), position), (shards_of,), jnp.float32, smallest / len(cuts), top_value / len(cuts))
        return jnp.repeat(jnp.exp(heights), dims[position] // shards_of).reshape((-1,) + (1,) * (len(dims) - position - 1))

    level = one(*cuts[0])
    for cut in cuts[1:]:
        level = level * one(*cut)
    return level


def routed_block(key, own, number, rows, amount, top, bound, lean):
    sequence = jax.random.permutation(key, amount)
    packed, usual = shares(amount, rows * top, bound, lean, True), shares(amount, rows * top, bound, lean, False)
    places = jnp.arange(amount)

    def named(tallies, offset_by):
        used = int((tallies > 0).sum())
        fixed = max(1, used // 4)
        passed = fixed + (places - fixed + offset_by * (used - fixed)) % max(1, amount - fixed)
        return jnp.zeros((amount,), jnp.int32).at[sequence[jnp.where(places < fixed, places, passed)]].set(jnp.asarray(tallies, jnp.int32))

    tallies = jnp.where(number % 4 == 0, named(packed, number // 4), named(usual, number - number // 4 - 1))
    mixed = jax.random.permutation(jax.random.fold_in(own, 3), amount)
    donor, taker = mixed[0:amount // 2 * 2:2], mixed[1:amount // 2 * 2:2]
    room = jnp.minimum(tallies[donor] - 1, bound - tallies[taker]) // 2
    room = jnp.where((donor == sequence[0]) | (taker == sequence[0]) | (tallies[taker] == 0), 0, jnp.maximum(room, 0))
    passed = jax.random.randint(jax.random.fold_in(own, 4), (amount // 2,), 0, 1 << 20) % (room + 1)
    tallies = tallies.at[donor].add(-passed).at[taker].add(passed)
    labels = jnp.searchsorted(jnp.cumsum(tallies), jnp.arange(rows * top), side="right").astype(jnp.int32)
    listing = labels.reshape(top, rows).T
    listing = listing[jax.random.permutation(jax.random.fold_in(own, 1), rows)]
    offset_by = jax.random.randint(jax.random.fold_in(own, 2), (rows, 1), 0, top)
    return jnp.take_along_axis(listing, (jnp.arange(top)[None, :] + offset_by) % top, axis=1)


def shares(count, total, limit, skew, full):
    portions = [(1 << 20) // math.isqrt(grade ** skew) + 1 for grade in range(1, count + 1)]
    largest = limit if full else min(limit, max(-(-total // count), total * portions[0] // sum(portions)))
    least = 1 if total - largest >= count - 1 else 0
    holding, spare = [largest] + [least] * (count - 1), total - largest - least * (count - 1)
    while spare > 0:
        free = [i for i in range(1, count) if holding[i] < largest] or [i for i in range(1, count) if holding[i] < limit]
        mass, remaining = sum([portions[i] for i in free]), spare
        for i in free:
            more = min(limit - holding[i], max(1, remaining * portions[i] // mass), spare)
            holding[i] = holding[i] + more
            spare = spare - more
    return np.array(holding)


def noise(stream_key, dims, scale, most, shards=(), held_as=jnp.bfloat16):
    entries = scale * jax.random.normal(stream_key, dims, jnp.float32)
    if shards:
        entries = entries * steps_of(stream_key, dims, shards, -0.22, 0.18)
    return jnp.clip(entries, -most, most).astype(held_as)


def setup_inputs(seed: int = 0) -> dict:
    arg_keys = jax.random.split(jax.random.key(seed), 7)
    tokens = noise(arg_keys[0], (TOKENS, D), 1.0, 6.0, ((0, 32),))
    expert_ids_keys = jax.random.split(jax.random.fold_in(arg_keys[1], 1), TOKENS // TOK_DEV)
    expert_ids_turns = jax.random.permutation(jax.random.fold_in(arg_keys[1], 3), TOKENS // TOK_DEV)
    expert_ids = jax.vmap(lambda own, number: routed_block(jax.random.fold_in(arg_keys[1], 2), own, number, TOK_DEV, EXPERTS, TOP, CAP, 2))(expert_ids_keys, expert_ids_turns).reshape((TOKENS, TOP))
    route_weights = jnp.clip(jnp.exp(math.log(0.4) - 2.5902672 * jax.random.uniform(arg_keys[2], (TOKENS, TOP), jnp.float32) ** steps_of(arg_keys[2], (TOKENS, TOP), ((0, 32),), -0.2, 0.2)), 0.03, 0.4)
    w_gate = noise(arg_keys[3], (EXPERTS, D, FFE), D ** -0.5, 0.125, ((0, 32),))
    w_up = noise(arg_keys[4], (EXPERTS, D, FFE), D ** -0.5, 0.125, ((0, 32),))
    w_down = noise(arg_keys[5], (EXPERTS, FFE, D), FFE ** -0.5, 0.21875, ((0, 32),))
    return {"tokens": tokens, "expert_ids": expert_ids, "route_weights": route_weights, "w_gate": w_gate, "w_up": w_up, "w_down": w_down}


def expert_ffn(rows, gate_proj, up_proj, down_proj):
    gate = jnp.dot(rows, gate_proj, preferred_element_type=jnp.float32)
    upper = jnp.dot(rows, up_proj, preferred_element_type=jnp.float32)
    hidden = (jax.nn.silu(gate) * upper).astype(jnp.bfloat16)
    return jnp.dot(hidden, down_proj, preferred_element_type=jnp.float32).astype(jnp.bfloat16)


def reference(tokens, expert_ids, route_weights, w_gate, w_up, w_down):
    blocks = TOKENS // TOK_DEV
    block_pairs = TOK_DEV * TOP
    flat_ids = expert_ids.reshape(blocks, block_pairs).astype(jnp.int32)
    onehot = (flat_ids[:, :, None] == jnp.arange(EXPERTS, dtype=jnp.int32)[None, None, :]).astype(jnp.int32)
    earlier = jnp.cumsum(onehot, axis=1) - onehot
    slot_index = jnp.sum(earlier * onehot, axis=2).astype(jnp.int32)
    owner = jnp.arange(blocks, dtype=jnp.int32)[:, None]
    keys = ((flat_ids * blocks + owner) * CAP + slot_index).reshape(-1).astype(jnp.int32)
    token_of = (jnp.arange(TOKENS * TOP, dtype=jnp.int32) // TOP).astype(jnp.int32)
    per_expert = blocks * CAP
    table_token = jnp.full((EXPERTS * per_expert,), -1, jnp.int32).at[keys].set(token_of)
    table_weight = jnp.zeros((EXPERTS * per_expert,), jnp.float32).at[keys].set(route_weights.reshape(-1))

    def one_expert(total, inputs):
        gate_proj, up_proj, down_proj, expert = inputs
        start = (expert * per_expert).astype(jnp.int32)
        index = lax.dynamic_slice_in_dim(table_token, start, per_expert)
        weight = lax.dynamic_slice_in_dim(table_weight, start, per_expert)
        safe = jnp.maximum(index, 0).astype(jnp.int32)
        rows = jnp.where((index >= 0)[:, None], tokens[safe], jnp.zeros((), tokens.dtype))
        output = expert_ffn(rows, gate_proj, up_proj, down_proj)
        total = total.at[safe].add(weight[:, None] * output.astype(jnp.float32))
        return total, None

    start_total = jnp.zeros((TOKENS, D), jnp.float32)
    total, _ = lax.scan(one_expert, start_total, (w_gate, w_up, w_down, jnp.arange(EXPERTS, dtype=jnp.int32)))
    return total.astype(jnp.bfloat16)
```

```python
import jax
import jax.numpy as jnp
from jax import lax
from jax.sharding import PartitionSpec as P

AXES = ("side", "lane")


def on_device(tokens, expert_ids, route_weights, w_gate, w_up, w_down):
    tok_rows, width = tokens.shape
    top_count = expert_ids.shape[1]
    device_count = lax.axis_size("side") * lax.axis_size("lane")
    capacity = 2 * tok_rows * top_count // device_count
    experts = jnp.arange(device_count, dtype=jnp.int32)
    weight = jnp.sum(
        jnp.where(expert_ids[:, :, None] == experts[None, None, :], route_weights[:, :, None], 0.0),
        axis=1,
    )
    me = lax.axis_index("side") * lax.axis_size("lane") + lax.axis_index("lane")
    every = lax.all_gather(tokens, AXES, axis=0, tiled=True).reshape(device_count, tok_rows, width)
    weights = lax.all_to_all(weight.T, AXES, split_axis=0, concat_axis=0, tiled=True)
    chosen = weights > 0.0
    counted = chosen.astype(jnp.int32)
    slot = jnp.cumsum(counted, axis=1) - counted
    table = (slot[:, None, :] == jnp.arange(capacity, dtype=jnp.int32)[None, :, None]) & chosen[
        :, None, :
    ]
    pick = table.astype(jnp.bfloat16)
    rows = jnp.einsum("bst,btd->bsd", pick, every, preferred_element_type=jnp.float32).astype(
        jnp.bfloat16
    )
    rows = rows.reshape(device_count * capacity, width)
    gate = jnp.dot(rows, w_gate[0], preferred_element_type=jnp.float32)
    upper = jnp.dot(rows, w_up[0], preferred_element_type=jnp.float32)
    hidden = (jax.nn.silu(gate) * upper).astype(jnp.bfloat16)
    output = jnp.dot(hidden, w_down[0], preferred_element_type=jnp.float32).astype(jnp.bfloat16)
    output = output.reshape(device_count, capacity, width)
    back = (pick.astype(jnp.float32) * weights[:, None, :]).astype(jnp.bfloat16)
    part = jnp.einsum("bst,bsd->btd", back, output, preferred_element_type=jnp.float32).astype(
        jnp.bfloat16
    )
    part = part.reshape(device_count * tok_rows, width)
    return lax.psum_scatter(part, AXES, scatter_dimension=0, tiled=True)


def solution(mesh):
    placed = (
        P(AXES, None),
        P(AXES, None),
        P(AXES, None),
        P(AXES, None, None),
        P(AXES, None, None),
        P(AXES, None, None),
    )
    return jax.shard_map(
        on_device, mesh=mesh, in_specs=placed, out_specs=P(AXES, None), check_vma=False
    )
```

```python
import functools

import jax
import jax.numpy as jnp
from jax import lax
from jax.experimental import pallas as pl
from jax.experimental.pallas import tpu as pltpu
from jax.sharding import PartitionSpec as P

AXES = ("side", "lane")
MESH = pl.DeviceIdType.MESH
BF16 = jnp.bfloat16
F32 = jnp.float32


def flip(value, mask):
    bit = 1
    out = value
    while bit <= mask:
        if mask & bit:
            out = out + bit - 2 * bit * ((value // bit) % 2)
        bit *= 2
    return out


def place(levels):
    side = lax.axis_index("side")
    level = lax.axis_index("lane")
    return side // 2, side % 2, level


def greet(devices):
    barrier = pltpu.get_barrier_semaphore()
    for device in devices:
        pl.semaphore_signal(barrier, inc=1, device_id=device, device_id_type=MESH)
    pl.semaphore_wait(barrier, len(devices))


def gather_kernel(
    levels, tokens, mine, wg, wu, wd, every, shares, wg2, wu2, wd2, send, recv, ssend, srecv, wsend, wrecv, local
):
    col, core, level = place(levels)
    half = tokens.shape[0] // 2
    chips = every.shape[0]
    col_x, col_y = flip(col, 1), flip(col, 2)
    dev_x, dev_y = (col_x * 2 + core, level), (col_y * 2 + core, level)
    twin = (col * 2 + 1 - core, level)
    me = col * levels + level
    others = [
        (flip(col, m // levels), flip(level, m % levels)) for m in range(1, chips)
    ]
    greet([(q * 2 + core, z) for q, z in others] + [twin])

    started = []

    def go(src, dst, s, r, device):
        copy = pltpu.make_async_remote_copy(
            src_ref=src, dst_ref=dst, send_sem=s, recv_sem=r, device_id=device, device_id_type=MESH
        )
        copy.start()
        started.append(copy)
        return copy

    for i, (q, z) in enumerate(others):
        go(mine.at[q * levels + z], shares.at[me], ssend.at[i], srecv.at[i], (q * 2 + core, z))
    keep = [
        pltpu.make_async_copy(tokens, every.at[me], local.at[0]),
        pltpu.make_async_copy(mine.at[me], shares.at[me], local.at[1]),
    ]
    for copy in keep:
        copy.start()

    lanes = []
    top, low = pl.ds(0, half), pl.ds(half, half)
    waited = set()
    for k in range(levels):
        z = flip(level, k)
        b = col * levels + z
        if k:
            lanes[k - 1].wait_recv()
            waited.add(id(lanes[k - 1]))
            block = every.at[b]
        else:
            block = tokens
        a = go(block.at[top], every.at[b, top], send.at[1, k], recv.at[1, k], dev_x)
        c = go(block.at[low], every.at[b, low], send.at[2, k], recv.at[2, k], dev_y)
        if k == 0:
            for m in range(1, levels):
                lanes.append(
                    go(tokens, every.at[me], send.at[0, m], recv.at[0, m], (col * 2 + core, flip(level, m)))
                )
        go(block.at[low], every.at[b, low], send.at[3, k], recv.at[3, k], dev_x)
        go(block.at[top], every.at[b, top], send.at[4, k], recv.at[4, k], dev_y)
        if k == 0:
            go(wg, wg2, wsend.at[0], wrecv.at[0], twin)
            go(wu, wu2, wsend.at[1], wrecv.at[1], twin)
            go(wd, wd2, wsend.at[2], wrecv.at[2], twin)
        a.wait_recv()
        waited.add(id(a))
        bx = every.at[col_x * levels + z, top]
        go(bx, bx, send.at[5, k], recv.at[5, k], dev_y)
        c.wait_recv()
        waited.add(id(c))
        by = every.at[col_y * levels + z, low]
        go(by, by, send.at[6, k], recv.at[6, k], dev_x)
    for copy in started:
        if id(copy) not in waited:
            copy.wait_recv()
        copy.wait_send()
    for copy in keep:
        copy.wait()


def return_kernel(levels, part, out, first, second, third, fold, level_sum, send, recv):
    col, core, level = place(levels)
    rows = out.shape[0]
    half = rows // 2
    col_x, col_y, col_xy = flip(col, 1), flip(col, 2), flip(flip(col, 1), 2)
    dev_x, dev_y = (col_x * 2 + core, level), (col_y * 2 + core, level)
    greet([dev_x, dev_y] + [(col * 2 + core, flip(level, m)) for m in range(1, levels)])
    top, low = pl.ds(0, half), pl.ds(half, half)
    started = []

    def go(src, dst, i, k, device):
        copy = pltpu.make_async_remote_copy(
            src_ref=src,
            dst_ref=dst,
            send_sem=send.at[i, k],
            recv_sem=recv.at[i, k],
            device_id=device,
            device_id_type=MESH,
        )
        copy.start()
        started.append(copy)
        return copy

    def add(dst, one, two):
        dst[...] = (one[...].astype(F32) + two[...].astype(F32)).astype(BF16)

    def stage_one(k):
        z = flip(level, k)
        return [
            go(part.at[col_xy * levels + z, top], first.at[k, 0, 0], 0, k, dev_x),
            go(part.at[col_xy * levels + z, low], first.at[k, 1, 0], 1, k, dev_y),
            go(part.at[col_x * levels + z, top], first.at[k, 0, 1], 2, k, dev_x),
            go(part.at[col_y * levels + z, low], first.at[k, 1, 1], 3, k, dev_y),
        ]

    def stage_two(k, ones):
        z = flip(level, k)
        ones[0].wait_recv()
        add(fold.at[k, 0], part.at[col_y * levels + z, top], first.at[k, 0, 0])
        a = go(fold.at[k, 0], second.at[k, 0], 4, k, dev_y)
        ones[1].wait_recv()
        add(fold.at[k, 1], part.at[col_x * levels + z, low], first.at[k, 1, 0])
        b = go(fold.at[k, 1], second.at[k, 1], 5, k, dev_x)
        return [a, b]

    def stage_three(k, ones, twos):
        z = flip(level, k)
        for copy in ones[2:] + twos:
            copy.wait_recv()
        for h, piece in enumerate((top, low)):
            level_sum[k, piece] = (
                part[col * levels + z, piece].astype(F32)
                + first[k, h, 1].astype(F32)
                + second[k, h].astype(F32)
            ).astype(BF16)
        if k:
            return go(level_sum.at[k], third.at[k], 6, k, (col * 2 + core, flip(level, k)))

    order = list(range(levels - 1, -1, -1))
    ones, twos, threes = {}, {}, {}
    ones[order[0]] = stage_one(order[0])
    for n, k in enumerate(order):
        if n + 1 < levels:
            ones[order[n + 1]] = stage_one(order[n + 1])
        twos[k] = stage_two(k, ones[k])
        if n:
            p = order[n - 1]
            threes[p] = stage_three(p, ones[p], twos[p])
    k = order[-1]
    stage_three(k, ones[k], twos[k])
    for m in range(1, levels):
        threes[m].wait_recv()
    total = level_sum[0].astype(F32)
    for m in range(1, levels):
        total = total + third[m].astype(F32)
    out[...] = total.astype(BF16)
    for copy in started:
        copy.wait_send()


def on_layers(levels, tokens, expert_ids, route_weights, w_gate, w_up, w_down):
    tok_rows, width = tokens.shape
    top_count = expert_ids.shape[1]
    device_count = lax.axis_size("side") * levels
    capacity = 2 * tok_rows * top_count // device_count
    chips = device_count // 2
    core = lax.axis_index("side") % 2
    experts = jnp.arange(device_count, dtype=jnp.int32)
    weight = jnp.sum(
        jnp.where(expert_ids[:, None, :] == experts[None, :, None], route_weights[:, None, :], 0.0),
        axis=2,
    ).T
    mine = weight.reshape(chips // levels, 2, levels, tok_rows).transpose(0, 2, 1, 3)
    mine = mine.reshape(chips, 2, tok_rows)
    mine = jnp.where(core == 1, mine[:, ::-1], mine)
    mine = jnp.pad(mine, ((0, 0), (0, 6), (0, 0)))
    anywhere = pl.BlockSpec(memory_space=pl.ANY)
    dma = pltpu.SemaphoreType.DMA
    shape = jax.ShapeDtypeStruct
    every, shares, wg2, wu2, wd2 = pl.pallas_call(
        functools.partial(gather_kernel, levels),
        out_shape=[
            shape((chips, tok_rows, width), BF16),
            shape(mine.shape, F32),
            shape(w_gate.shape, BF16),
            shape(w_up.shape, BF16),
            shape(w_down.shape, BF16),
        ],
        in_specs=[anywhere] * 5,
        out_specs=[anywhere] * 5,
        scratch_shapes=[
            dma((7, levels)),
            dma((7, levels)),
            dma((chips - 1,)),
            dma((chips - 1,)),
            dma((3,)),
            dma((3,)),
            dma((2,)),
        ],
        compiler_params=pltpu.CompilerParams(collective_id=0, has_side_effects=True),
        name="spread",
    )(tokens, mine, w_gate, w_up, w_down)

    weights = shares[:, :2]
    chosen = weights > 0.0
    before = jnp.triu(jnp.ones((tok_rows, tok_rows), BF16), 1)
    slot = jnp.dot(chosen.astype(BF16).reshape(chips * 2, tok_rows), before, preferred_element_type=F32)
    slot = slot.reshape(chips, 2, tok_rows).astype(jnp.int32)
    table = (
        slot[:, :, None, :] == jnp.arange(capacity, dtype=jnp.int32)[None, None, :, None]
    ) & chosen[:, :, None, :]
    pick = table.astype(BF16)
    outputs = []
    for i, (wg, wu, wd) in enumerate(((w_gate, w_up, w_down), (wg2, wu2, wd2))):
        rows = jnp.einsum("bst,btd->bsd", pick[:, i], every, preferred_element_type=F32).astype(BF16)
        rows = rows.reshape(chips * capacity, width)
        gate = jnp.dot(rows, wg[0], preferred_element_type=F32)
        upper = jnp.dot(rows, wu[0], preferred_element_type=F32)
        hidden = (jax.nn.silu(gate) * upper).astype(BF16)
        outputs.append(
            jnp.dot(hidden, wd[0], preferred_element_type=F32)
            .astype(BF16)
            .reshape(chips, capacity, width)
        )
    back = jnp.where(table, weights[:, :, None, :], 0.0).astype(BF16)
    back = back.reshape(chips, 2 * capacity, tok_rows)
    part = jnp.einsum(
        "bst,bsd->btd", back, jnp.concatenate(outputs, axis=1), preferred_element_type=F32
    ).astype(BF16)

    half = tok_rows // 2
    vmem = pl.BlockSpec(memory_space=pltpu.VMEM)
    return pl.pallas_call(
        functools.partial(return_kernel, levels),
        out_shape=shape((tok_rows, width), BF16),
        in_specs=[vmem],
        out_specs=vmem,
        scratch_shapes=[
            pltpu.VMEM((levels, 2, 2, half, width), BF16),
            pltpu.VMEM((levels, 2, half, width), BF16),
            pltpu.VMEM((levels, tok_rows, width), BF16),
            pltpu.VMEM((levels, 2, half, width), BF16),
            pltpu.VMEM((levels, tok_rows, width), BF16),
            dma((7, levels)),
            dma((7, levels)),
        ],
        compiler_params=pltpu.CompilerParams(
            collective_id=1, has_side_effects=True, vmem_limit_bytes=56 * 2**20
        ),
        name="collect",
    )(part)


def expert_ffn(rows, gate_proj, up_proj, down_proj):
    gate = jnp.dot(rows, gate_proj, preferred_element_type=jnp.float32)
    upper = jnp.dot(rows, up_proj, preferred_element_type=jnp.float32)
    hidden = (jax.nn.silu(gate) * upper).astype(jnp.bfloat16)
    return jnp.dot(hidden, down_proj, preferred_element_type=jnp.float32).astype(jnp.bfloat16)


def on_device(tokens, expert_ids, route_weights, w_gate, w_up, w_down):
    tok_rows = tokens.shape[0]
    width = tokens.shape[1]
    top_count = expert_ids.shape[1]
    side_count = lax.axis_size("side")
    device_count = side_count * lax.axis_size("lane")
    local_count = w_gate.shape[0]
    expert_count = device_count * local_count
    capacity = 2 * tok_rows * top_count // expert_count
    flat_ids = expert_ids.reshape(-1)
    onehot = (flat_ids[:, None] == jnp.arange(expert_count, dtype=jnp.int32)[None, :]).astype(
        jnp.int32
    )
    earlier = jnp.cumsum(onehot, axis=0) - onehot
    slot_index = jnp.sum(earlier * onehot, axis=1)
    position = (flat_ids * capacity + slot_index).reshape(tok_rows, top_count)
    buffer_rows = jnp.arange(expert_count * capacity, dtype=jnp.int32)
    dispatch_table = jnp.any(buffer_rows[:, None, None] == position[None, :, :], axis=2).astype(
        jnp.bfloat16
    )
    outgoing = jnp.dot(dispatch_table, tokens, preferred_element_type=jnp.float32).astype(
        jnp.bfloat16
    )
    outgoing = outgoing.reshape(expert_count, capacity, width)
    received = lax.all_to_all(outgoing, ("side", "lane"), split_axis=0, concat_axis=0, tiled=True)
    count = received.shape[1]
    grouped = received.reshape(device_count, local_count, count, width)
    rows = grouped[:, 0].reshape(device_count * count, width)
    output = expert_ffn(rows, w_gate[0], w_up[0], w_down[0])
    results = [output.reshape(device_count, count, width)]
    returned = lax.all_to_all(
        jnp.stack(results, axis=1).reshape(device_count * local_count, count, width),
        ("side", "lane"),
        split_axis=0,
        concat_axis=0,
        tiled=True,
    )
    flat_back = returned.reshape(expert_count * capacity, width)
    picked = flat_back[position]
    mixed = jnp.einsum("tk,tkd->td", route_weights, picked, preferred_element_type=jnp.float32)
    return mixed.astype(jnp.bfloat16)


def layered(mesh, tokens):
    side, levels = mesh.shape["side"], mesh.shape["lane"]
    layer_bytes = tokens.shape[0] // 2 * tokens.shape[1] * tokens.dtype.itemsize
    return side == 2**3 and levels & (levels - 1) == 0 and 3 * layer_bytes < 32 * 2**20


def solution(mesh):
    placed = (
        P(AXES, None),
        P(AXES, None),
        P(AXES, None),
        P(AXES, None, None),
        P(AXES, None, None),
        P(AXES, None, None),
    )

    def run(tokens, *rest):
        body = on_device
        if layered(mesh, tokens):
            body = functools.partial(on_layers, mesh.shape["lane"])
        return jax.shard_map(
            body, mesh=mesh, in_specs=placed, out_specs=P(AXES, None), check_vma=False
        )(tokens, *rest)

    return run
```

```python
import functools

import jax
import jax.numpy as jnp
from jax import lax
from jax.experimental import pallas as pl
from jax.experimental.pallas import tpu as pltpu
from jax.sharding import PartitionSpec as P

AXES = ("side", "lane")
MESH = pl.DeviceIdType.MESH
BF16 = jnp.bfloat16
F32 = jnp.float32


def flip(value, mask):
    bit = 1
    out = value
    while bit <= mask:
        if mask & bit:
            out = out + bit - 2 * bit * ((value // bit) % 2)
        bit *= 2
    return out


def place(levels):
    side = lax.axis_index("side")
    level = lax.axis_index("lane")
    return side // 2, side % 2, level


def greet(devices):
    barrier = pltpu.get_barrier_semaphore()
    for device in devices:
        pl.semaphore_signal(barrier, inc=1, device_id=device, device_id_type=MESH)
    pl.semaphore_wait(barrier, len(devices))


def gather_kernel(
    levels, tokens, mine, wg, wu, wd, every, shares, wg2, wu2, wd2, send, recv, ssend, srecv, wsend, wrecv, local
):
    col, core, level = place(levels)
    half = tokens.shape[0] // 2
    chips = every.shape[0]
    col_x, col_y = flip(col, 1), flip(col, 2)
    dev_x, dev_y = (col_x * 2 + core, level), (col_y * 2 + core, level)
    twin = (col * 2 + 1 - core, level)
    me = col * levels + level
    others = [
        (flip(col, m // levels), flip(level, m % levels)) for m in range(1, chips)
    ]
    greet([(q * 2 + core, z) for q, z in others] + [twin])

    started = []

    def go(src, dst, s, r, device):
        copy = pltpu.make_async_remote_copy(
            src_ref=src, dst_ref=dst, send_sem=s, recv_sem=r, device_id=device, device_id_type=MESH
        )
        copy.start()
        started.append(copy)
        return copy

    for i, (q, z) in enumerate(others):
        go(mine.at[q * levels + z], shares.at[me], ssend.at[i], srecv.at[i], (q * 2 + core, z))
    keep = [
        pltpu.make_async_copy(tokens, every.at[me], local.at[0]),
        pltpu.make_async_copy(mine.at[me], shares.at[me], local.at[1]),
    ]
    for copy in keep:
        copy.start()

    lanes = []
    top, low = pl.ds(0, half), pl.ds(half, half)
    waited = set()
    for k in range(levels):
        z = flip(level, k)
        b = col * levels + z
        if k:
            lanes[k - 1].wait_recv()
            waited.add(id(lanes[k - 1]))
            block = every.at[b]
        else:
            block = tokens
        a = go(block.at[top], every.at[b, top], send.at[1, k], recv.at[1, k], dev_x)
        c = go(block.at[low], every.at[b, low], send.at[2, k], recv.at[2, k], dev_y)
        if k == 0:
            for m in range(1, levels):
                lanes.append(
                    go(tokens, every.at[me], send.at[0, m], recv.at[0, m], (col * 2 + core, flip(level, m)))
                )
        go(block.at[low], every.at[b, low], send.at[3, k], recv.at[3, k], dev_x)
        go(block.at[top], every.at[b, top], send.at[4, k], recv.at[4, k], dev_y)
        if k == 0:
            go(wg, wg2, wsend.at[0], wrecv.at[0], twin)
            go(wu, wu2, wsend.at[1], wrecv.at[1], twin)
            go(wd, wd2, wsend.at[2], wrecv.at[2], twin)
        a.wait_recv()
        waited.add(id(a))
        bx = every.at[col_x * levels + z, top]
        go(bx, bx, send.at[5, k], recv.at[5, k], dev_y)
        c.wait_recv()
        waited.add(id(c))
        by = every.at[col_y * levels + z, low]
        go(by, by, send.at[6, k], recv.at[6, k], dev_x)
    for copy in started:
        if id(copy) not in waited:
            copy.wait_recv()
        copy.wait_send()
    for copy in keep:
        copy.wait()


def return_kernel(
    levels, every, pick, back, wga, wua, wda, wgb, wub, wdb, out, wgs, wus, wds, xs, ys, part, first,
    second, third, fold, level_sum, send, recv, fetch
):
    loads = [
        pltpu.make_async_copy(src.at[0], dst.at[e], fetch.at[i, e])
        for i, (dst, pair) in enumerate(((wgs, (wga, wgb)), (wus, (wua, wub)), (wds, (wda, wdb))))
        for e, src in enumerate(pair)
    ]
    for copy in loads:
        copy.start()
    col, core, level = place(levels)
    rows = out.shape[0]
    half = rows // 2
    col_x, col_y, col_xy = flip(col, 1), flip(col, 2), flip(flip(col, 1), 2)
    dev_x, dev_y = (col_x * 2 + core, level), (col_y * 2 + core, level)
    greet([dev_x, dev_y] + [(col * 2 + core, flip(level, m)) for m in range(1, levels)])
    top, low = pl.ds(0, half), pl.ds(half, half)
    started = []

    def go(src, dst, i, k, device):
        copy = pltpu.make_async_remote_copy(
            src_ref=src,
            dst_ref=dst,
            send_sem=send.at[i, k],
            recv_sem=recv.at[i, k],
            device_id=device,
            device_id_type=MESH,
        )
        copy.start()
        started.append(copy)
        return copy

    def add(dst, one, two):
        dst[...] = (one[...].astype(F32) + two[...].astype(F32)).astype(BF16)

    columns = every.shape[0] // levels
    slots = pick.shape[1] // 2

    def compute(k):
        z = flip(level, k)
        for j in range(columns):
            b = j * levels + z
            rows_b = jnp.dot(pick[b], every[b], preferred_element_type=F32).astype(BF16)
            for e in range(2):
                xs[e, pl.ds(j * slots, slots)] = rows_b[e * slots : (e + 1) * slots]

        def expert(e, carry):
            x = xs[e]
            gate = jnp.dot(x, wgs[e], preferred_element_type=F32)
            upper = jnp.dot(x, wus[e], preferred_element_type=F32)
            hidden = (gate / (1.0 + jnp.exp(-gate)) * upper).astype(BF16)
            ys[e] = jnp.dot(hidden, wds[e], preferred_element_type=F32).astype(BF16)
            return carry

        lax.fori_loop(0, 2, expert, 0)
        for j in range(columns):
            b = j * levels + z
            mix = back[b]
            y = jnp.concatenate([ys[e, pl.ds(j * slots, slots)] for e in range(2)], axis=0)
            part[b] = jnp.dot(mix, y, preferred_element_type=F32).astype(BF16)

    def stage_one(k):
        z = flip(level, k)
        return [
            go(part.at[col_xy * levels + z, top], first.at[k, 0, 0], 0, k, dev_x),
            go(part.at[col_xy * levels + z, low], first.at[k, 1, 0], 1, k, dev_y),
            go(part.at[col_x * levels + z, top], first.at[k, 0, 1], 2, k, dev_x),
            go(part.at[col_y * levels + z, low], first.at[k, 1, 1], 3, k, dev_y),
        ]

    def stage_two(k, ones):
        z = flip(level, k)
        ones[0].wait_recv()
        add(fold.at[k, 0], part.at[col_y * levels + z, top], first.at[k, 0, 0])
        a = go(fold.at[k, 0], second.at[k, 0], 4, k, dev_y)
        ones[1].wait_recv()
        add(fold.at[k, 1], part.at[col_x * levels + z, low], first.at[k, 1, 0])
        b = go(fold.at[k, 1], second.at[k, 1], 5, k, dev_x)
        return [a, b]

    def stage_three(k, ones, twos):
        z = flip(level, k)
        for copy in ones[2:] + twos:
            copy.wait_recv()
        for h, piece in enumerate((top, low)):
            level_sum[k, piece] = (
                part[col * levels + z, piece].astype(F32)
                + first[k, h, 1].astype(F32)
                + second[k, h].astype(F32)
            ).astype(BF16)
        if k:
            return go(level_sum.at[k], third.at[k], 6, k, (col * 2 + core, flip(level, k)))

    order = list(range(levels - 1, -1, -1))
    ones, twos, threes = {}, {}, {}
    for copy in loads:
        copy.wait()
    for n in range(levels + 2):
        if n < levels:
            compute(order[n])
            ones[order[n]] = stage_one(order[n])
        if 1 <= n <= levels:
            p = order[n - 1]
            twos[p] = stage_two(p, ones[p])
        if n >= 2:
            p = order[n - 2]
            threes[p] = stage_three(p, ones[p], twos[p])
    for m in range(1, levels):
        threes[m].wait_recv()
    total = level_sum[0].astype(F32)
    for m in range(1, levels):
        total = total + third[m].astype(F32)
    out[...] = total.astype(BF16)
    for copy in started:
        copy.wait_send()


def on_layers(levels, tokens, expert_ids, route_weights, w_gate, w_up, w_down):
    tok_rows, width = tokens.shape
    top_count = expert_ids.shape[1]
    device_count = lax.axis_size("side") * levels
    capacity = 2 * tok_rows * top_count // device_count
    chips = device_count // 2
    core = lax.axis_index("side") % 2
    experts = jnp.arange(device_count, dtype=jnp.int32)
    weight = jnp.sum(
        jnp.where(expert_ids[:, None, :] == experts[None, :, None], route_weights[:, None, :], 0.0),
        axis=2,
    ).T
    mine = weight.reshape(chips // levels, 2, levels, tok_rows).transpose(0, 2, 1, 3)
    mine = mine.reshape(chips, 2, tok_rows)
    mine = jnp.where(core == 1, mine[:, ::-1], mine)
    mine = jnp.pad(mine, ((0, 0), (0, 6), (0, 0)))
    anywhere = pl.BlockSpec(memory_space=pl.ANY)
    dma = pltpu.SemaphoreType.DMA
    shape = jax.ShapeDtypeStruct
    every, shares, wg2, wu2, wd2 = pl.pallas_call(
        functools.partial(gather_kernel, levels),
        out_shape=[
            shape((chips, tok_rows, width), BF16),
            shape(mine.shape, F32),
            shape(w_gate.shape, BF16),
            shape(w_up.shape, BF16),
            shape(w_down.shape, BF16),
        ],
        in_specs=[anywhere] * 5,
        out_specs=[anywhere] * 5,
        scratch_shapes=[
            dma((7, levels)),
            dma((7, levels)),
            dma((chips - 1,)),
            dma((chips - 1,)),
            dma((3,)),
            dma((3,)),
            dma((2,)),
        ],
        compiler_params=pltpu.CompilerParams(collective_id=0, has_side_effects=True),
        name="spread",
    )(tokens, mine, w_gate, w_up, w_down)

    weights = shares[:, :2]
    chosen = weights > 0.0
    before = jnp.triu(jnp.ones((tok_rows, tok_rows), BF16), 1)
    slot = jnp.dot(chosen.astype(BF16).reshape(chips * 2, tok_rows), before, preferred_element_type=F32)
    slot = slot.reshape(chips, 2, tok_rows).astype(jnp.int32)
    table = (
        slot[:, :, None, :] == jnp.arange(capacity, dtype=jnp.int32)[None, None, :, None]
    ) & chosen[:, :, None, :]
    pick = table.astype(BF16)
    back = jnp.where(table, weights[:, :, None, :], 0.0).astype(BF16)
    back = back.reshape(chips, 2 * capacity, tok_rows).transpose(0, 2, 1)
    pick = pick.reshape(chips, 2 * capacity, tok_rows)
    half = tok_rows // 2
    vmem = pl.BlockSpec(memory_space=pltpu.VMEM)
    return pl.pallas_call(
        functools.partial(return_kernel, levels),
        out_shape=shape((tok_rows, width), BF16),
        in_specs=[vmem] * 3 + [anywhere] * 6,
        out_specs=vmem,
        scratch_shapes=[
            pltpu.VMEM((2,) + w_gate.shape[1:], BF16),
            pltpu.VMEM((2,) + w_up.shape[1:], BF16),
            pltpu.VMEM((2,) + w_down.shape[1:], BF16),
            pltpu.VMEM((2, chips // levels * capacity, width), BF16),
            pltpu.VMEM((2, chips // levels * capacity, width), BF16),
            pltpu.VMEM((chips, tok_rows, width), BF16),
            pltpu.VMEM((levels, 2, 2, half, width), BF16),
            pltpu.VMEM((levels, 2, half, width), BF16),
            pltpu.VMEM((levels, tok_rows, width), BF16),
            pltpu.VMEM((levels, 2, half, width), BF16),
            pltpu.VMEM((levels, tok_rows, width), BF16),
            dma((7, levels)),
            dma((7, levels)),
            dma((3, 2)),
        ],
        compiler_params=pltpu.CompilerParams(
            collective_id=1, has_side_effects=True, vmem_limit_bytes=60 * 2**20
        ),
        name="collect",
    )(every, pick, back, w_gate, w_up, w_down, wg2, wu2, wd2)


def expert_ffn(rows, gate_proj, up_proj, down_proj):
    gate = jnp.dot(rows, gate_proj, preferred_element_type=jnp.float32)
    upper = jnp.dot(rows, up_proj, preferred_element_type=jnp.float32)
    hidden = (jax.nn.silu(gate) * upper).astype(jnp.bfloat16)
    return jnp.dot(hidden, down_proj, preferred_element_type=jnp.float32).astype(jnp.bfloat16)


def on_device(tokens, expert_ids, route_weights, w_gate, w_up, w_down):
    tok_rows = tokens.shape[0]
    width = tokens.shape[1]
    top_count = expert_ids.shape[1]
    side_count = lax.axis_size("side")
    device_count = side_count * lax.axis_size("lane")
    local_count = w_gate.shape[0]
    expert_count = device_count * local_count
    capacity = 2 * tok_rows * top_count // expert_count
    flat_ids = expert_ids.reshape(-1)
    onehot = (flat_ids[:, None] == jnp.arange(expert_count, dtype=jnp.int32)[None, :]).astype(
        jnp.int32
    )
    earlier = jnp.cumsum(onehot, axis=0) - onehot
    slot_index = jnp.sum(earlier * onehot, axis=1)
    position = (flat_ids * capacity + slot_index).reshape(tok_rows, top_count)
    buffer_rows = jnp.arange(expert_count * capacity, dtype=jnp.int32)
    dispatch_table = jnp.any(buffer_rows[:, None, None] == position[None, :, :], axis=2).astype(
        jnp.bfloat16
    )
    outgoing = jnp.dot(dispatch_table, tokens, preferred_element_type=jnp.float32).astype(
        jnp.bfloat16
    )
    outgoing = outgoing.reshape(expert_count, capacity, width)
    received = lax.all_to_all(outgoing, ("side", "lane"), split_axis=0, concat_axis=0, tiled=True)
    count = received.shape[1]
    grouped = received.reshape(device_count, local_count, count, width)
    rows = grouped[:, 0].reshape(device_count * count, width)
    output = expert_ffn(rows, w_gate[0], w_up[0], w_down[0])
    results = [output.reshape(device_count, count, width)]
    returned = lax.all_to_all(
        jnp.stack(results, axis=1).reshape(device_count * local_count, count, width),
        ("side", "lane"),
        split_axis=0,
        concat_axis=0,
        tiled=True,
    )
    flat_back = returned.reshape(expert_count * capacity, width)
    picked = flat_back[position]
    mixed = jnp.einsum("tk,tkd->td", route_weights, picked, preferred_element_type=jnp.float32)
    return mixed.astype(jnp.bfloat16)


def layered(mesh, tokens):
    side, levels = mesh.shape["side"], mesh.shape["lane"]
    layer_bytes = tokens.shape[0] // 2 * tokens.shape[1] * tokens.dtype.itemsize
    return side == 2**3 and levels & (levels - 1) == 0 and 3 * layer_bytes < 32 * 2**20


def solution(mesh):
    placed = (
        P(AXES, None),
        P(AXES, None),
        P(AXES, None),
        P(AXES, None, None),
        P(AXES, None, None),
        P(AXES, None, None),
    )

    def run(tokens, *rest):
        body = on_device
        if layered(mesh, tokens):
            body = functools.partial(on_layers, mesh.shape["lane"])
        return jax.shard_map(
            body, mesh=mesh, in_specs=placed, out_specs=P(AXES, None), check_vma=False
        )(tokens, *rest)

    return run
```
